32 devices in a mesh: dp: 2 (over x), expert: 16 (over z, y, core).
Axes of the slice: x: 2, y: 2, z: 4, core: 2. Of those that a mesh axis runs over, the one named last changes fastest.
Arguments:
- tokens_in: bfloat16 [4096, 2880], P(('dp', 'expert')), may hold values from -6 to 6
- grad_out: bfloat16 [4096, 2880], P(('dp', 'expert')), may hold values from -6 to 6
- expert_ids: int32 [4096, 4], P(('dp', 'expert')), may hold values from 0 to 15, all different within a row; in each aligned block of 128 rows (0 to 127, 128 to 255, ...) at most 40 rows name the same one
- combine_weights: float32 [4096, 4], P(('dp', 'expert')), may hold values from 0.1 to 1
- up_weight: bfloat16 [16, 2880, 1440], P('expert'), may hold values from -0.109375 to 0.109375
- down_weight: bfloat16 [16, 1440, 2880], P('expert'), may hold values from -0.15625 to 0.15625
Outputs:
- grad_input: bfloat16 [4096, 2880], P(('dp', 'expert'))
- grad_up: bfloat16 [16, 2880, 1440], P('expert', 'dp')
- grad_down: bfloat16 [16, 1440, 2880], P('expert', 'dp')
The draws below stay inside these ranges and needn't reach their ends.
Inputs may be any that keep to these rules, and one draw needn't show every extreme that they name: `expert_ids`: each row names 4 different experts; in the rows of one device no expert is named by more than 40 rows, a bound that some block reaches.
All inputs are finite; a program needn't handle non-finite values.
Results may differ from the reference program's by a relative error of at most 0.0064.
Values may be sent and summed in bfloat16 or wider, within the bound.
A program may use at most 192 MiB of HBM per device.

```python
import math
import jax
import jax.numpy as jnp
import numpy as np
from jax import lax

D = 2880
F = 1440
TOPK = 4
TOK_DEV = 128
EXPERTS = 16
CAP = 40
TOKENS = 4096
N_DP = 2
N_EXPERT = 16


def level_of(key, dims, pieces, smallest, top_value):
    factor_of, own = 1.0, jax.random.fold_in(key, 6)
    for dim, blocks in pieces:
        steps = jnp.exp(jax.random.uniform(jax.random.fold_in(own, dim), (blocks,), jnp.float32, smallest / len(pieces), top_value / len(pieces)))
        factor_of = factor_of * jnp.repeat(steps, dims[dim] // blocks).reshape([-1 if axis == dim else 1 for axis in range(len(dims))])
    return factor_of


def deal_out(rng, own, number, rows, amount, top, reach, skew):
    ranking = jax.random.permutation(rng, amount)
    crowded, ordinary = portions_of(amount, rows * top, reach, skew, True), portions_of(amount, rows * top, reach, skew, False)
    places = jnp.arange(amount)

    def named(tallies, turn):
        used = int((tallies > 0).sum())
        fixed = max(1, used // 4)
        passed = fixed + (places - fixed + turn * (used - fixed)) % max(1, amount - fixed)
        return jnp.zeros((amount,), jnp.int32).at[ranking[jnp.where(places < fixed, places, passed)]].set(jnp.asarray(tallies, jnp.int32))

    tallies = jnp.where(number % 4 == 0, named(crowded, number // 4), named(ordinary, number - number // 4 - 1))
    mixed = jax.random.permutation(jax.random.fold_in(own, 3), amount)
    source_of, taker = mixed[0:amount // 2 * 2:2], mixed[1:amount // 2 * 2:2]
    margin = jnp.minimum(tallies[source_of] - 1, reach - tallies[taker]) // 2
    margin = jnp.where((source_of == ranking[0]) | (taker == ranking[0]) | (tallies[taker] == 0), 0, jnp.maximum(margin, 0))
    passed = jax.random.randint(jax.random.fold_in(own, 4), (amount // 2,), 0, 1 << 20) % (margin + 1)
    tallies = tallies.at[source_of].add(-passed).at[taker].add(passed)
    labels = jnp.searchsorted(jnp.cumsum(tallies), jnp.arange(rows * top), side="right").astype(jnp.int32)
    table = labels.reshape(top, rows).T
    table = table[jax.random.permutation(jax.random.fold_in(own, 1), rows)]
    turn = jax.random.randint(jax.random.fold_in(own, 2), (rows, 1), 0, top)
    return jnp.take_along_axis(table, (jnp.arange(top)[None, :] + turn) % top, axis=1)


def portions_of(amount, total, reach, skew, full):
    portions = [(1 << 20) // math.isqrt(standing ** skew) + 1 for standing in range(1, amount + 1)]
    largest = reach if full else min(reach, max(-(-total // amount), total * portions[0] // sum(portions)))
    least = 1 if total - largest >= amount - 1 else 0
    counts, surplus = [largest] + [least] * (amount - 1), total - largest - least * (amount - 1)
    while surplus > 0:
        movable = [i for i in range(1, amount) if counts[i] < largest] or [i for i in range(1, amount) if counts[i] < reach]
        mass, remaining = sum([portions[i] for i in movable]), surplus
        for i in movable:
            extra = min(reach - counts[i], max(1, remaining * portions[i] // mass), surplus)
            counts[i] = counts[i] + extra
            surplus = surplus - extra
    return np.array(counts)


def bell_draw(own_key, dims, deviation, bound, shards=(), kind=jnp.bfloat16):
    array = jax.random.normal(own_key, dims, jnp.float32) * deviation
    if len(shards) > 0:
        array = level_of(own_key, dims, shards, -0.22, 0.18) * array
    return jnp.clip(array, min=-bound, max=bound).astype(kind)


def setup_inputs(seed: int = 0) -> dict:
    key_list = jax.random.split(jax.random.key(seed), 7)
    tokens_in = bell_draw(key_list[0], (TOKENS, D), 1.0, 6.0, ((0, 32),))
    grad_out = bell_draw(key_list[1], (TOKENS, D), 1.0, 6.0, ((0, 32),))
    expert_ids_keys = jax.random.split(jax.random.fold_in(key_list[2], 1), TOKENS // TOK_DEV)
    expert_ids_turns = jax.random.permutation(jax.random.fold_in(key_list[2], 3), TOKENS // TOK_DEV)
    expert_ids = jax.vmap(lambda own, number: deal_out(jax.random.fold_in(key_list[2], 2), own, number, TOK_DEV, EXPERTS, TOPK, CAP, 1))(expert_ids_keys, expert_ids_turns).reshape((TOKENS, TOPK))
    combine_weights = jnp.clip(jnp.exp(math.log(1.0) - 2.3025851 * jax.random.uniform(key_list[3], (TOKENS, TOPK), jnp.float32) ** level_of(key_list[3], (TOKENS, TOPK), ((0, 32),), -0.2, 0.2)), 0.1, 1.0)
    up_weight = bell_draw(key_list[4], (EXPERTS, D, F), D ** -0.5, 0.109375, ((0, 16),))
    down_weight = bell_draw(key_list[5], (EXPERTS, F, D), F ** -0.5, 0.15625, ((0, 16),))
    return dict(tokens_in=tokens_in, grad_out=grad_out, expert_ids=expert_ids, combine_weights=combine_weights, up_weight=up_weight, down_weight=down_weight)


def silu_parts(preact):
    logistic = jax.nn.sigmoid(preact)
    return preact * logistic, logistic * (1.0 + preact * (1.0 - logistic))


def reference(tokens_in, grad_out, expert_ids, combine_weights, up_weight, down_weight):
    model_width = tokens_in.shape[1]
    devices_all = N_DP * N_EXPERT
    block_rows = TOK_DEV * TOPK
    per_expert = devices_all * CAP
    routed = TOKENS * TOPK
    flat_ids = expert_ids.reshape(devices_all, block_rows)
    one_hot = (flat_ids[:, :, None] == jnp.arange(EXPERTS, dtype=jnp.int32)[None, None, :]).astype(jnp.int32)
    slot_rank = jnp.sum((jnp.cumsum(one_hot, axis=1) - one_hot) * one_hot, axis=2)
    source_dev = jnp.arange(devices_all, dtype=jnp.int32)[:, None]
    position = (flat_ids * per_expert + source_dev * CAP + slot_rank).reshape(-1).astype(jnp.int32)
    slot_table = jnp.full((EXPERTS * per_expert,), routed, jnp.int32).at[position].set(jnp.arange(routed, dtype=jnp.int32))
    padded_x = jnp.concatenate([tokens_in, jnp.zeros((1, model_width), tokens_in.dtype)], axis=0)
    padded_dy = jnp.concatenate([grad_out, jnp.zeros((1, model_width), grad_out.dtype)], axis=0)
    padded_weight = jnp.concatenate([combine_weights.reshape(-1), jnp.zeros((1,), combine_weights.dtype)], axis=0)

    def one_expert(operands):
        rows_idx, w_up, w_down = operands
        source_token = rows_idx // TOPK
        rows_x = padded_x[source_token]
        rows_grad = (padded_weight[rows_idx][:, None] * padded_dy[source_token].astype(jnp.float32)).astype(jnp.bfloat16)
        preact = jnp.dot(rows_x, w_up, preferred_element_type=jnp.float32)
        activated, slope = silu_parts(preact)
        activated = activated.astype(jnp.bfloat16)
        grad_act = jnp.dot(rows_grad, w_down.T, preferred_element_type=jnp.float32)
        grad_pre = (grad_act * slope).astype(jnp.bfloat16)
        grad_rows = jnp.dot(grad_pre, w_up.T, preferred_element_type=jnp.float32).astype(jnp.bfloat16)
        grad_upper = jnp.dot(rows_x.T, grad_pre, preferred_element_type=jnp.float32).astype(jnp.bfloat16)
        grad_lower = jnp.dot(activated.T, rows_grad, preferred_element_type=jnp.float32).astype(jnp.bfloat16)
        return grad_rows, grad_upper, grad_lower

    grad_rows, grad_up, grad_down = lax.map(one_expert, (slot_table.reshape(EXPERTS, per_expert), up_weight, down_weight))
    picked = grad_rows.reshape(-1, model_width)[position].reshape(TOKENS, TOPK, model_width)
    grad_input = jnp.sum(picked.astype(jnp.float32), axis=1).astype(jnp.bfloat16)
    return grad_input, grad_up, grad_down
```

```python
import functools
import jax
import jax.numpy as jnp
from jax import lax
from jax.experimental import pallas as pl
from jax.experimental.pallas import tpu as pltpu
from jax.sharding import PartitionSpec as P

MESH = pl.DeviceIdType.MESH
LANES = 512


def silu_parts(preact):
    logistic = jax.nn.sigmoid(preact)
    return (preact * logistic, logistic * (1.0 + preact * (1.0 - logistic)))


def contract_rows(left, right):
    return lax.dot_general(
        left, right, (((0,), (0,)), ((), ())), preferred_element_type=jnp.float32
    )


def contract_cols(left, right):
    return lax.dot_general(
        left, right, (((1,), (1,)), ((), ())), preferred_element_type=jnp.float32
    )


def other_replica(value):
    pairs = lax.axis_size("dp")
    return lax.ppermute(value, "dp", [(i, (i + 1) % pairs) for i in range(pairs)])


def grid_of(experts):
    inner = 1
    while (2 * inner) ** 2 <= experts and experts % (2 * inner) == 0:
        inner *= 2
    return experts // inner, inner


def pieces(width, step=LANES):
    return [(at, min(step, width - at)) for at in range(0, width, step)]


def positions_of(expert_ids, experts_all, capacity):
    token_count = expert_ids.shape[0]
    hits = expert_ids[:, :, None] == jnp.arange(experts_all, dtype=jnp.int32)[None, None, :]
    chosen = jnp.any(hits, axis=1).astype(jnp.bfloat16)
    token_index = jnp.arange(token_count, dtype=jnp.int32)
    earlier = (token_index[None, :] < token_index[:, None]).astype(jnp.bfloat16)
    rank = jnp.dot(earlier, chosen, preferred_element_type=jnp.float32)
    slot_rank = jnp.sum(jnp.where(hits, rank[:, None, :], 0.0), axis=2)
    return expert_ids.astype(jnp.float32) * capacity + slot_rank


class Place:
    def __init__(self, outer, inner):
        self.outer, self.inner = outer, inner
        self.replica = lax.axis_index("dp")
        self.replicas = lax.axis_size("dp")
        self.expert = lax.axis_index("expert")
        self.level = self.expert // inner
        self.seat = self.expert % inner

    def at_level(self, level):
        return (self.replica, level * self.inner + self.seat)

    def at_seat(self, seat):
        return (self.replica, self.level * self.inner + seat)

    def twin(self):
        return (lax.rem(self.replica + 1, self.replicas), self.expert)

    def nth(self, i):
        z, last = self.level, self.outer - 1
        low = jnp.minimum(z, last - z)
        near = z + ((i + 1) // 2) * (1 if i % 2 else -1)
        far = jnp.where(z <= last - z, z + (i - low), z - (i - low))
        return jnp.where(i <= 2 * low, near, far)

    def onward(self, source):
        step = jnp.where(source < self.level, 1, -1)
        target = self.level + step
        valid = jnp.logical_and(target >= 0, target < self.outer)
        return jnp.clip(target, 0, self.outer - 1), valid

    def greet(self):
        barrier = pltpu.get_barrier_semaphore()
        for k in range(1, self.outer):
            level = lax.rem(self.level + k, self.outer)
            pl.semaphore_signal(barrier, inc=1, device_id=self.at_level(level), device_id_type=MESH)
        for k in range(1, self.inner):
            seat = lax.rem(self.seat + k, self.inner)
            pl.semaphore_signal(barrier, inc=1, device_id=self.at_seat(seat), device_id_type=MESH)
        pl.semaphore_signal(barrier, inc=1, device_id=self.twin(), device_id_type=MESH)
        pl.semaphore_wait(barrier, self.outer + self.inner - 1)


def remote(src, dst, send, recv, device):
    return pltpu.make_async_remote_copy(
        src_ref=src, dst_ref=dst, send_sem=send, recv_sem=recv, device_id=device, device_id_type=MESH
    )


def hits_of(place, route, cap, top, seat, seats=1):
    rows = seats * cap
    tokens = route.shape[-1]
    base = ((place.level * place.inner + seat) * cap).astype(jnp.float32)
    slot = base + lax.broadcasted_iota(jnp.int32, (rows, tokens), 0).astype(jnp.float32)
    taken = jnp.zeros((rows, tokens), jnp.float32)
    weight = jnp.zeros((rows, tokens), jnp.float32)
    for k in range(top):
        match = slot == route[k : k + 1, :]
        taken = jnp.where(match, 1.0, taken)
        weight = jnp.where(match, route[top + k : top + k + 1, :], weight)
    return taken.astype(jnp.bfloat16), jnp.sum(weight, axis=1, keepdims=True)


def dispatch_kernel(
    outer, inner, cap, top,
    g_ref, x_ref, route_ref,
    rows_g, rows_x, other_g, routes,
    gline, xline, gsel, xsel,
    r_send, r_recv, z_send, z_recv, y_send, y_recv, d_send, d_recv,
):
    place = Place(outer, inner)
    level, seat = place.level, place.seat
    lines, sels, rows, owns = (gline, xline), (gsel, xsel), (rows_g, rows_x), (g_ref, x_ref)
    width = g_ref.shape[-1]
    place.greet()

    def route_copy(k):
        target = lax.rem(level + k, outer)
        return remote(route_ref, routes.at[level], r_send.at[k], r_recv.at[level], place.at_level(target))

    def route_arrival(source):
        return remote(route_ref, routes.at[source], r_send.at[0], r_recv.at[source], place.at_level(level))

    for k in range(1, outer):
        route_copy(k).start()

    def own_copy(t, side):
        target = jnp.clip(level + side, 0, outer - 1)
        valid = level > 0 if side < 0 else level < outer - 1
        which = 0 if side < 0 else 1
        copy = remote(owns[t], lines[t].at[level], z_send.at[t, 0, which], z_recv.at[t, level], place.at_level(target))
        return copy, valid

    def on_copy(t, i):
        source = place.nth(i)
        target, valid = place.onward(source)
        copy = remote(
            lines[t].at[source], lines[t].at[source], z_send.at[t, i, 0], z_recv.at[t, source], place.at_level(target)
        )
        return copy, valid

    for t in (0, 1):
        for side in (1, -1):
            copy, valid = own_copy(t, side)
            pl.when(valid)(copy.start)

    def seat_copy(t, i, source, k):
        to = lax.rem(seat + k, inner)
        return remote(
            sels[t].at[i, to], rows[t].at[source, seat], y_send.at[t, i, k], y_recv.at[t, source, seat], place.at_seat(to)
        )

    def own_rows(t, i, source):
        return pltpu.make_async_copy(sels[t].at[i, seat], rows[t].at[source, seat], y_recv.at[t, source, seat])

    def arrivals(t, i, source):
        own_rows(t, i, source).wait()
        for k in range(1, inner):
            other = lax.rem(seat + k, inner)
            remote(
                sels[t].at[i, other], rows[t].at[source, other], y_send.at[t, i, k], y_recv.at[t, source, other],
                place.at_seat(other),
            ).wait_recv()

    def twin_copy(i, source):
        return remote(rows_g.at[source], other_g.at[source], d_send.at[i], d_recv.at[source], place.twin())

    def choose(t, i, source, value, route):
        whole = cap % 8 == 0
        groups = [(0, inner)] if whole else [(q, 1) for q in range(inner)]
        for first, seats in groups:
            taken, weight = hits_of(place, route, cap, top, first, seats)
            for at, size in pieces(width):
                picked = jnp.dot(taken, value[:, at : at + size], preferred_element_type=jnp.float32)
                if t == 0:
                    picked = picked * weight
                for q in range(seats):
                    sels[t][i, first + q, :, at : at + size] = picked[q * cap : (q + 1) * cap].astype(jnp.bfloat16)
        for k in range(1, inner):
            seat_copy(t, i, source, k).start()
        own_rows(t, i, source).start()

    routes[level] = route_ref[...]
    for t in (0, 1):
        choose(t, 0, level, owns[t], route_ref[...])

    pending = [(0, level)]
    for first in range(1, outer, 2):
        group = [i for i in (first, first + 1) if i < outer]
        for t in (0, 1):
            for i in group:
                source = place.nth(i)
                copy, valid = on_copy(t, i)
                copy.wait_recv()
                pl.when(valid)(copy.start)
                if t == 0:
                    route_arrival(source).wait_recv()
                choose(t, i, source, lines[t].at[source], routes[source])
                if pending:
                    j, was = pending.pop(0)
                    arrivals(0, j, was)
                    twin_copy(j, was).start()
                if t == 0:
                    pending.append((i, source))
    for j, was in pending:
        arrivals(0, j, was)
        twin_copy(j, was).start()
    for i in range(outer):
        source = level if i == 0 else place.nth(i)
        arrivals(1, i, source)

    for k in range(1, outer):
        route_copy(k).wait_send()
    for t in (0, 1):
        for side in (1, -1):
            copy, valid = own_copy(t, side)
            pl.when(valid)(copy.wait_send)
        for i in range(1, outer):
            copy, valid = on_copy(t, i)
            pl.when(valid)(copy.wait_send)
        for i in range(outer):
            source = level if i == 0 else place.nth(i)
            for k in range(1, inner):
                seat_copy(t, i, source, k).wait_send()
    for i in range(outer):
        source = level if i == 0 else place.nth(i)
        copy = twin_copy(i, source)
        copy.wait_send()
        copy.wait_recv()


def dispatch(g, x, route, outer, inner, cap, top):
    tokens, width = g.shape
    dtype = g.dtype
    rows = jax.ShapeDtypeStruct((outer, inner, cap, width), dtype)
    sem = pltpu.SemaphoreType.DMA
    vmem, hbm = pl.BlockSpec(memory_space=pltpu.VMEM), pl.BlockSpec(memory_space=pl.ANY)
    return pl.pallas_call(
        functools.partial(dispatch_kernel, outer, inner, cap, top),
        name="dispatch",
        out_shape=(rows, rows, rows, jax.ShapeDtypeStruct((outer,) + route.shape, route.dtype)),
        in_specs=[vmem, vmem, vmem],
        out_specs=(hbm, hbm, hbm, vmem),
        scratch_shapes=[
            pltpu.VMEM((outer, tokens, width), dtype),
            pltpu.VMEM((outer, tokens, width), dtype),
            pltpu.VMEM((outer, inner, cap, width), dtype),
            pltpu.VMEM((outer, inner, cap, width), dtype),
            sem((outer,)), sem((outer,)),
            sem((2, outer, 2)), sem((2, outer)),
            sem((2, outer, inner)), sem((2, outer, inner)),
            sem((outer,)), sem((outer,)),
        ],
        compiler_params=pltpu.CompilerParams(
            collective_id=0, has_side_effects=True, vmem_limit_bytes=48 * 1024 * 1024
        ),
    )(g, x, route)


def return_kernel(
    outer, inner, cap, top,
    rows, routes, out,
    back, incoming, going, acc,
    y_send, y_recv, z_send, z_recv,
):
    place = Place(outer, inner)
    level, seat = place.level, place.seat
    width = out.shape[-1]
    place.greet()
    order = [place.nth(i) for i in range(outer - 1, 0, -1)] + [level]

    def seat_copy(i, k):
        to = lax.rem(seat + k, inner)
        return remote(
            rows.at[order[i], to], back.at[order[i], seat], y_send.at[i, k], y_recv.at[order[i], seat], place.at_seat(to)
        )

    def own_rows(i):
        return pltpu.make_async_copy(rows.at[order[i], seat], back.at[order[i], seat], y_recv.at[order[i], seat])

    def arrivals(i):
        own_rows(i).wait()
        for k in range(1, inner):
            other = lax.rem(seat + k, inner)
            remote(
                rows.at[order[i], other], back.at[order[i], other], y_send.at[i, k], y_recv.at[order[i], other],
                place.at_seat(other),
            ).wait_recv()

    for i in range(outer):
        for k in range(1, inner):
            seat_copy(i, k).start()
        own_rows(i).start()

    def onward(i):
        target = order[i]
        up = target > level
        side = jnp.where(up, 0, 1)
        to = jnp.clip(jnp.where(up, level + 1, level - 1), 0, outer - 1)
        return remote(going.at[i], incoming.at[side, target], z_send.at[i], z_recv.at[side, target], place.at_level(to))

    def coming(side, target):
        return remote(
            going.at[0], incoming.at[side, target], z_send.at[0], z_recv.at[side, target], place.at_level(level)
        )

    def summed(i, at, size):
        route = routes[order[i]]
        total = None
        for q in range(inner):
            taken, _ = hits_of(place, route, cap, top, q)
            part = contract_rows(taken, back[order[i], q, :, at : at + size])
            total = part if total is None else total + part
        return total

    def reaches(target):
        up = target > level
        return jnp.where(up, 0, 1), jnp.where(up, level > 0, level < outer - 1)

    for i in range(outer - 1):
        side, exists = reaches(order[i])
        pl.when(jnp.logical_not(exists))(functools.partial(clear, incoming, side, order[i]))

    for i in range(outer - 1):
        target = order[i]
        side, exists = reaches(target)
        arrivals(i)
        for at, size in pieces(width):
            acc[:, at : at + size] = summed(i, at, size)
        pl.when(exists)(coming(side, target).wait_recv)
        going[i] = (acc[...] + incoming[side, target].astype(jnp.float32)).astype(jnp.bfloat16)
        onward(i).start()

    arrivals(outer - 1)
    for side, exists in ((0, level > 0), (1, level < outer - 1)):
        pl.when(exists)(coming(side, level).wait_recv)
        pl.when(jnp.logical_not(exists))(functools.partial(clear, incoming, side, level))
    for at, size in pieces(width):
        total = summed(outer - 1, at, size)
        for side in (0, 1):
            total = total + incoming[side, level, :, at : at + size].astype(jnp.float32)
        out[:, at : at + size] = total.astype(jnp.bfloat16)

    for i in range(outer):
        for k in range(1, inner):
            seat_copy(i, k).wait_send()
        if i < outer - 1:
            onward(i).wait_send()


def clear(ref, side, level):
    ref[side, level] = jnp.zeros(ref.shape[2:], ref.dtype)


def give_back(rows, routes, tokens, outer, inner, cap, top):
    width = rows.shape[-1]
    sem = pltpu.SemaphoreType.DMA
    vmem, hbm = pl.BlockSpec(memory_space=pltpu.VMEM), pl.BlockSpec(memory_space=pl.ANY)
    return pl.pallas_call(
        functools.partial(return_kernel, outer, inner, cap, top),
        name="give_back",
        out_shape=jax.ShapeDtypeStruct((tokens, width), rows.dtype),
        in_specs=[hbm, vmem],
        out_specs=vmem,
        scratch_shapes=[
            pltpu.VMEM((outer, inner, cap, width), rows.dtype),
            pltpu.VMEM((2, outer, tokens, width), rows.dtype),
            pltpu.VMEM((outer, tokens, width), rows.dtype),
            pltpu.VMEM((tokens, width), jnp.float32),
            sem((outer, inner)), sem((outer, inner)),
            sem((outer,)), sem((2, outer)),
        ],
        compiler_params=pltpu.CompilerParams(
            collective_id=1, has_side_effects=True, vmem_limit_bytes=48 * 1024 * 1024
        ),
    )(rows, routes)


def local(tokens_in, grad_out, expert_ids, combine_weights, up_weight, down_weight):
    token_count, model_width = tokens_in.shape
    top_count = expert_ids.shape[1]
    experts_all = lax.axis_size("expert") * up_weight.shape[0]
    capacity = 5 * token_count * top_count // (4 * experts_all)
    outer, inner = grid_of(experts_all)
    w_up = up_weight[0]
    w_down = down_weight[0]
    replica = lax.axis_index("dp")

    def halves(value):
        half = value.shape[1] // 2
        low, high = value[:, :half], value[:, half:]
        first = replica == 0
        return jnp.where(first, low, high), jnp.where(first, high, low)

    position = positions_of(expert_ids, experts_all, capacity)
    route = jnp.concatenate([position.T, combine_weights.T], axis=0)
    sizes = (outer, inner, capacity, top_count)
    rows_grad, rows_x, other_grad, routes = dispatch(grad_out, tokens_in, route, *sizes)
    flat = (experts_all * capacity, model_width)
    rows_grad, rows_x, other_grad = (v.reshape(flat) for v in (rows_grad, rows_x, other_grad))
    keep_x, give_x = halves(rows_x)
    other_x = other_replica(give_x)
    grad_act = contract_cols(rows_grad, w_down)
    preact = jnp.dot(rows_x, w_up, preferred_element_type=jnp.float32)
    activated, slope = silu_parts(preact)
    activated = activated.astype(jnp.bfloat16)
    grad_pre = (grad_act * slope).astype(jnp.bfloat16)
    keep_act, give_act = halves(activated)
    other_act = other_replica(give_act)
    other_pre = other_replica(grad_pre)
    grad_rows = contract_cols(grad_pre, w_up).astype(jnp.bfloat16)
    shape = (outer, inner, capacity, model_width)
    grad_input = give_back(grad_rows.reshape(shape), routes, token_count, *sizes)
    grad_down = contract_rows(keep_act, rows_grad) + contract_rows(other_act, other_grad)
    grad_up = contract_rows(keep_x, grad_pre) + contract_rows(other_x, other_pre)
    return (grad_input, grad_up.astype(jnp.bfloat16)[None], grad_down.astype(jnp.bfloat16)[None])


def solution(mesh):
    return jax.shard_map(
        local,
        mesh=mesh,
        in_specs=(
            P(("dp", "expert"), None),
            P(("dp", "expert"), None),
            P(("dp", "expert"), None),
            P(("dp", "expert"), None),
            P("expert", None, None),
            P("expert", None, None),
        ),
        out_specs=(P(("dp", "expert"), None), P("expert", "dp", None), P("expert", "dp", None)),
        check_vma=False,
    )
```
